32 devices in a mesh: row: 2 (over core), col: 8 (over z, x), grp: 2 (over y).
Axes of the slice: x: 2, y: 2, z: 4, core: 2. Of those that a mesh axis runs over, the one named last changes fastest.
Arguments:
- momentum: float32 [2, 4096, 16384], P('grp', 'row', 'col'), may hold values from -6 to 6
- gradient: bfloat16 [2, 4096, 16384], P('grp', 'row', 'col'), may hold values from -6 to 6
- factor_q: float32 [2, 16384, 256], P('grp', 'col', 'row'), may hold values from -0.046875 to 0.046875
- weights: float32 [2, 4096, 16384], P(None, 'row', ('col', 'grp')), may hold values from -6 to 6
- tokens: bfloat16 [256, 4096], P(None, 'row'), may hold values from -0.08984375 to 0.08984375
Outputs:
- momentum_out: float32 [2, 4096, 16384], P('grp', 'row', 'col')
- factor_out: float32 [2, 16384, 256], P('grp', 'col', 'row')
- weights_out: float32 [2, 4096, 16384], P(None, 'row', ('col', 'grp'))
- hidden: bfloat16 [256, 16384], P('row', ('col', 'grp'))
The draws below stay inside these ranges and needn't reach their ends.
All inputs are finite; a program needn't handle non-finite values.
Results may differ from the reference program's by a relative error of at most 0.0061.
Values may be sent and summed in bfloat16 or wider, within the bound.
No kernel may reach another device: no remote copies, remote signals or barrier semaphores. Data moves between devices by JAX's collectives and lax.ppermute only.
A program may use at most 128 MiB of HBM per device.

```python
import math
import jax
import jax.numpy as jnp
from jax import lax

D = 4096
HID = 16384
RANK = 256
BATCH = 256


def level_of(rng, extent, pieces, smallest, largest):
    level = 1.0
    for axis_at, shards_of in pieces:
        steps = jax.random.uniform(jax.random.fold_in(jax.random.fold_in(rng, 6), axis_at), (shards_of,), jnp.float32, smallest / len(pieces), largest / len(pieces))
        level = level * jnp.repeat(jnp.exp(steps), extent[axis_at] // shards_of).reshape((-1,) + (1,) * (len(extent) - 1 - axis_at))
    return level


def normal_values(stream_key, extent, width, bound, cuts=(), dtype=jnp.bfloat16):
    drawn = jax.random.normal(stream_key, extent, jnp.float32) * width
    if len(cuts) > 0:
        drawn = level_of(stream_key, extent, cuts, -0.22, 0.18) * drawn
    return jnp.clip(drawn, min=-bound, max=bound).astype(dtype)


def setup_inputs(seed: int = 0) -> dict:
    arg_keys = jax.random.split(jax.random.key(seed), 6)
    momentum = normal_values(arg_keys[0], (2, D, HID), 1.0, 6.0, ((0, 2), (1, 2), (2, 8)), jnp.float32)
    gradient = normal_values(arg_keys[1], (2, D, HID), 1.0, 6.0, ((0, 2), (1, 2), (2, 8)))
    factor_q = normal_values(arg_keys[2], (2, HID, RANK), HID ** -0.5, 0.046875, ((0, 2), (1, 8), (2, 2)), jnp.float32)
    weights = normal_values(arg_keys[3], (2, D, HID), 1.0, 6.0, ((1, 2), (2, 16)), jnp.float32)
    tokens = normal_values(arg_keys[4], (BATCH, D), 0.015625, 0.08984375, ((1, 2),))
    return {"momentum": momentum, "gradient": gradient, "factor_q": factor_q, "weights": weights, "tokens": tokens}


feedback = 0.05
epsilon = 1e-06

def reference(momentum, gradient, factor_q, weights, tokens):
    step_size = 0.4 * math.sqrt(max(D, HID))
    mom_list = []
    q_list = []
    weight_list = []
    act_list = []
    for which in range(2):
        buffer = momentum[which] + gradient[which].astype(jnp.float32)
        buffer_h = buffer.astype(jnp.bfloat16)
        q_h = factor_q[which].astype(jnp.bfloat16)
        raw_left = jnp.dot(buffer_h.astype(jnp.float32), q_h.astype(jnp.float32), preferred_element_type=jnp.float32)
        gram_sum = jnp.dot(raw_left.T, raw_left, precision=lax.Precision.HIGHEST)
        factor_l = jnp.linalg.cholesky(gram_sum)
        ortho_left = jax.scipy.linalg.solve_triangular(factor_l, raw_left.T, lower=True).T
        left_h = ortho_left.astype(jnp.bfloat16)
        right_full = jnp.dot(buffer_h.T.astype(jnp.float32), left_h.astype(jnp.float32), preferred_element_type=jnp.float32)
        right_h = right_full.astype(jnp.bfloat16)
        mom_list.append(buffer - feedback * jnp.dot(left_h.astype(jnp.float32), right_h.T.astype(jnp.float32), preferred_element_type=jnp.float32))
        col_norms = jnp.sqrt(lax.optimization_barrier(jnp.sum(right_full * right_full, axis=0)) + epsilon)
        new_q = right_full / col_norms
        q_list.append(new_q)
        new_q_h = new_q.astype(jnp.bfloat16)
        new_weight = weights[which] - step_size * jnp.dot(left_h.astype(jnp.float32), new_q_h.T.astype(jnp.float32), preferred_element_type=jnp.float32)
        weight_list.append(new_weight)
        act_list.append(jnp.dot(tokens.astype(jnp.float32), new_weight.astype(jnp.bfloat16).astype(jnp.float32), preferred_element_type=jnp.float32))
    hidden = (jax.nn.silu(act_list[0]) * act_list[1]).astype(jnp.bfloat16)
    return (jnp.stack(mom_list), jnp.stack(q_list), jnp.stack(weight_list), hidden)
```

```python
import functools
import math

import jax
import jax.numpy as jnp
from jax import lax
from jax.experimental import pallas as pl
from jax.experimental.pallas import tpu as pltpu
from jax.sharding import PartitionSpec as P


feedback = 0.05
epsilon = 1e-06

f32 = jnp.float32
bf16 = jnp.bfloat16


def peers(n, k):
    return [(i, i ^ k) for i in range(n)]


def bits_of(n):
    assert n & (n - 1) == 0
    return [1 << b for b in range(n.bit_length() - 1)]


def gather_blocks(x, axis, n, at, dim):
    for k in bits_of(n):
        other = lax.ppermute(x, axis, peers(n, k))
        upper = (at & k) != 0
        x = jnp.concatenate([jnp.where(upper, other, x), jnp.where(upper, x, other)], axis=dim)
    return x


def sum_over(x, axis, n, wire=f32):
    for k in bits_of(n):
        x = x + lax.ppermute(x.astype(wire), axis, peers(n, k)).astype(f32)
    return x


def send_all(blocks, axis, n):
    return [lax.ppermute(blocks[k], axis, peers(n, k)) for k in range(1, n)]


def stacked(x, order):
    one = x.astype(bf16)
    rest = x - one.astype(f32)
    two = rest.astype(bf16)
    pieces = (one, two, (rest - two.astype(f32)).astype(bf16))
    return jnp.concatenate([pieces[i] for i in order], axis=0)


def chol_inv_kernel(at_ref, g_ref, out_ref, part_ref, s_ref):
    n = g_ref.shape[0]
    b = 16
    s_ref[:, :n] = g_ref[...]
    s_ref[:, n:] = (
        lax.broadcasted_iota(jnp.int32, (n, n), 0) == lax.broadcasted_iota(jnp.int32, (n, n), 1)
    ).astype(f32)
    rows = lax.broadcasted_iota(jnp.int32, (b, 128), 0)
    for r0 in range(0, n, b):
        lo = r0 // 128 * 128
        hi = n + (r0 + b + 127) // 128 * 128
        tiles = [s_ref[r0 : r0 + b, t : t + 128] for t in range(lo, hi, 128)]
        cols = [
            jnp.broadcast_to(tiles[0][:, r0 - lo + j : r0 - lo + j + 1], (b, 128)) for j in range(b)
        ]
        scale = None
        for i in range(b):
            piv = jnp.broadcast_to(cols[i][i : i + 1, :], (b, 128))
            scale = piv if scale is None else jnp.where(rows == i, piv, scale)
            if i + 1 < b:
                ratio = jnp.where(rows > i, cols[i], 0.0) * (1.0 / piv)
                for j in range(i + 1, b):
                    cols[j] = cols[j] - ratio * cols[j][i : i + 1, :]
                tiles = [t - ratio * t[i : i + 1, :] for t in tiles]
        scale = lax.rsqrt(scale)
        tiles = [t * scale for t in tiles]
        if r0 + b < n:
            upper = jnp.concatenate(tiles, axis=1)
            upd = dot(
                stacked(upper[:, : n - lo], (0, 0, 1, 0, 1, 2)).T,
                stacked(upper, (0, 1, 0, 2, 1, 0)),
            )
            s_ref[r0 + b :, lo:hi] = s_ref[r0 + b :, lo:hi] - upd[r0 + b - lo :, :]
        for k, t in enumerate(range(lo, hi, 128)):
            if t >= n:
                out_ref[r0 : r0 + b, t - n : t - n + 128] = tiles[k]
        for t in range(hi, 2 * n, 128):
            out_ref[r0 : r0 + b, t - n : t - n + 128] = jnp.zeros((b, 128), f32)
    rows = part_ref.shape[0]
    part_ref[...] = out_ref[pl.ds(pl.multiple_of(at_ref[0] * rows, rows), rows), :]


def chol_inv(place, gram, shares):
    n = gram.shape[0]
    return pl.pallas_call(
        chol_inv_kernel,
        out_shape=(pltpu.VMEM((n, n), f32), pltpu.VMEM((n // shares, n), f32)),
        in_specs=[SM, VM],
        out_specs=(VM, VM),
        scratch_shapes=[pltpu.VMEM((n, 2 * n), f32)],
        compiler_params=params(6),
        name="chol_inv",
    )(place, gram)


def split(x):
    hi = x.astype(bf16)
    return hi, (x - hi.astype(f32)).astype(bf16)


def dot_t(a, b):
    return lax.dot_general(a, b, (((1,), (1,)), ((), ())), preferred_element_type=f32)


def dot(a, b):
    return jnp.dot(a, b, preferred_element_type=f32)


VM = pl.BlockSpec(memory_space=pltpu.VMEM)
SM = pl.BlockSpec(memory_space=pltpu.SMEM)
HB = pl.BlockSpec(memory_space=pltpu.HBM)
DMA = pltpu.SemaphoreType.DMA


def params(mib):
    return pltpu.CompilerParams(vmem_limit_bytes=mib << 20)


def rows_per_step(width):
    return min(256, width)


def load_kernel(at_ref, m_ref, g_ref, q_ref, buf_ref, left_ref, grad_ref, sem_m, sem_g):
    width = buf_ref.shape[0]
    _, size, _ = left_ref.shape
    ch = rows_per_step(width)
    copies = []
    for i in range(width // ch):
        at = pl.ds(i * ch, ch)
        pair = (
            pltpu.make_async_copy(m_ref.at[at], buf_ref.at[at], sem_m.at[i]),
            pltpu.make_async_copy(g_ref.at[at], grad_ref.at[at], sem_g.at[i]),
        )
        for c in pair:
            c.start()
        copies.append(pair)
    for i, pair in enumerate(copies):
        at = pl.ds(i * ch, ch)
        for c in pair:
            c.wait()
        buf = buf_ref[at, :] + grad_ref[at, :].astype(f32)
        buf_ref[at, :] = buf
        part = dot(buf.astype(bf16), q_ref[...]).astype(bf16)
        for r in range(0, ch, size):
            left_ref[at_ref[1] ^ ((i * ch + r) // size)] = part[r : r + size, :]


def load_left(place, m, g, q, blocks):
    width, hid = m.shape
    n = width // rows_per_step(width)
    assert rows_per_step(width) % (width // blocks) == 0
    return pl.pallas_call(
        load_kernel,
        out_shape=(
            pltpu.VMEM((width, hid), f32),
            pltpu.VMEM((blocks, width // blocks, q.shape[1]), bf16),
        ),
        in_specs=[SM, HB, HB, VM],
        out_specs=(VM, VM),
        scratch_shapes=[pltpu.VMEM((width, hid), bf16), DMA((n,)), DMA((n,))],
        compiler_params=params(16),
        name="load_left",
    )(place, in_hbm(m), in_hbm(g), q)


def in_hbm(x):
    return pltpu.with_memory_space_constraint(x, pltpu.HBM)


def fetch_kernel(at_ref, w_ref, after_ref, out_ref, sem):
    copies = []
    ch = rows_per_step(w_ref.shape[1])
    for i in range(w_ref.shape[1] // ch):
        at = pl.ds(i * ch, ch)
        copies.append(
            pltpu.make_async_copy(w_ref.at[at_ref[2], at], out_ref.at[at], sem.at[i])
        )
    for c in copies:
        c.start()
    for c in copies:
        c.wait()


def fetch(place, w, after):
    n = w.shape[1] // rows_per_step(w.shape[1])
    return pl.pallas_call(
        fetch_kernel,
        out_shape=pltpu.VMEM(w.shape[1:], w.dtype),
        in_specs=[SM, HB, VM],
        out_specs=VM,
        scratch_shapes=[DMA((n,))],
        compiler_params=params(1),
        name="fetch_weights",
    )(place, w, after)


def sum_kernel(*refs):
    total = refs[0][...].astype(f32)
    for r in refs[1:-1]:
        total = total + r[...].astype(f32)
    refs[-1][...] = total.astype(bf16)


def block_sum(blocks):
    return pl.pallas_call(
        sum_kernel,
        out_shape=pltpu.VMEM(blocks[0].shape, bf16),
        in_specs=[VM] * len(blocks),
        out_specs=VM,
        compiler_params=params(4),
        name="block_sum",
    )(*blocks)


def gram_kernel(at_ref, *refs):
    blocks, raw_ref, gram_ref = refs[:-2], refs[-2], refs[-1]
    size = blocks[0].shape[0]
    for k, r in enumerate(blocks):
        start = pl.multiple_of((at_ref[1] ^ k) * size, size)
        raw_ref[pl.ds(start, size), :] = r[...]
    raw = raw_ref[...]
    gram_ref[...] = lax.dot_general(
        raw, raw, (((0,), (0,)), ((), ())), preferred_element_type=f32
    )


def join_gram(place, blocks):
    size, rank = blocks[0].shape
    return pl.pallas_call(
        gram_kernel,
        out_shape=(pltpu.VMEM((size * len(blocks), rank), bf16), pltpu.VMEM((rank, rank), f32)),
        in_specs=[SM] + [VM] * len(blocks),
        out_specs=(VM, VM),
        compiler_params=params(6),
        name="join_gram",
    )(place, *blocks)


def right_kernel(raw_ref, buf_ref, out_ref, outh_ref):
    raw_t = raw_ref[...].T
    hid = buf_ref.shape[1]
    ch = min(256, hid)
    for i in range(hid // ch):
        at = pl.ds(i * ch, ch)
        part = dot(raw_t, buf_ref[:, at].astype(bf16))
        out_ref[:, at] = part
        outh_ref[:, at] = part.astype(bf16)


def raw_right(raw, buf):
    shape = (raw.shape[1], buf.shape[1])
    return pl.pallas_call(
        right_kernel,
        out_shape=(pltpu.VMEM(shape, f32), pltpu.VMEM(shape, bf16)),
        in_specs=[VM, VM],
        out_specs=(VM, VM),
        compiler_params=params(6),
        name="raw_right",
    )(raw, buf)


def factors_kernel(
    at_ref, raw_ref, inv_ref, rr_ref, rro_ref, left_ref, right_ref, righth_ref, own_ref, part_ref, sq_ref,
    split_ref,
):
    inv_hi, inv_lo = split(inv_ref[...])
    left_ref[...] = (dot_t(raw_ref[...], inv_hi) + dot_t(raw_ref[...], inv_lo)).astype(bf16)
    hid = rr_ref.shape[1]
    half = split_ref.shape[2]
    ch = min(512, half)
    total = jnp.zeros((rr_ref.shape[0], 1), f32)
    for i in range(hid // ch):
        at = pl.ds(i * ch, ch)
        hi, lo = split(rr_ref[:, at] + rro_ref[:, at].astype(f32))
        right = dot(inv_hi, hi) + dot(inv_lo, hi) + dot(inv_hi, lo)
        right_ref[:, at] = right
        right_h = right.astype(bf16)
        righth_ref[:, at] = right_h
        split_ref[at_ref[2] ^ (i * ch // half), :, pl.ds(i * ch % half, ch)] = right_h
        total = total + jnp.sum(right * right, axis=1, keepdims=True)
    own_ref[...] = split_ref[0]
    rows = part_ref.shape[0]
    part_ref[...] = split_ref[1, pl.ds(pl.multiple_of(at_ref[0] * rows, rows), rows), :]
    sq_ref[...] = jnp.broadcast_to(total, (total.shape[0], 128)).T[: sq_ref.shape[0], :]


def factors(place, raw, inv_l, rr, rro, groups, shares):
    rank, hid = rr.shape
    return pl.pallas_call(
        factors_kernel,
        out_shape=(
            pltpu.VMEM(raw.shape, bf16),
            pltpu.VMEM((rank, hid), f32),
            pltpu.VMEM((rank, hid), bf16),
            pltpu.VMEM((rank, hid // groups), bf16),
            pltpu.VMEM((rank // shares, hid // groups), bf16),
            pltpu.VMEM((8, rank), f32),
        ),
        in_specs=[SM, VM, VM, VM, VM],
        out_specs=(VM, VM, VM, VM, VM, VM),
        scratch_shapes=[pltpu.VMEM((groups, rank, hid // groups), bf16)],
        compiler_params=params(6),
        name="factors",
    )(place, raw, inv_l, rr, rro)


def share_kernel(at_ref, right_ref, norm_ref, out_ref, col_ref):
    n = out_ref.shape[1]
    col_ref[...] = norm_ref[...].T
    at = pl.ds(pl.multiple_of(at_ref[0] * n, n), n)
    out_ref[...] = (right_ref[at, :] * col_ref[at, 0:1]).T


def factor_share(place, right, inv_norm, share):
    rank, hid = right.shape
    return pl.pallas_call(
        share_kernel,
        out_shape=jax.ShapeDtypeStruct((hid, share), f32),
        in_specs=[SM, VM, VM],
        out_specs=VM,
        scratch_shapes=[pltpu.VMEM((rank, 8), f32)],
        compiler_params=params(6),
        name="factor_share",
    )(place, right, inv_norm)


SLOTS = 4


def feedback_kernel(buf_ref, left_ref, right_ref, *rest, lo, hi, ch):
    out_ref, stage_ref, sem = rest[-3:]
    pending = []
    for i, r in enumerate(range(lo, hi, ch)):
        slot = i % SLOTS
        if i >= SLOTS:
            pending[i - SLOTS].wait()
        at = pl.ds(r, ch)
        stage_ref[slot] = buf_ref[at, :] - feedback * dot(left_ref[at, :], right_ref[...])
        copy = pltpu.make_async_copy(stage_ref.at[slot], out_ref.at[at], sem.at[slot])
        copy.start()
        pending.append(copy)
    for copy in pending[-SLOTS:]:
        copy.wait()


def apply_feedback(buf, left, right, out, lo, hi):
    width, hid = buf.shape
    ch = min(128, hi - lo)
    args = (buf, left, right) + (() if out is None else (out,))
    return pl.pallas_call(
        functools.partial(feedback_kernel, lo=lo, hi=hi, ch=ch),
        out_shape=pltpu.HBM((width, hid), f32),
        in_specs=[VM, VM, VM] + ([] if out is None else [HB]),
        out_specs=HB,
        input_output_aliases={} if out is None else {3: 0},
        scratch_shapes=[pltpu.VMEM((SLOTS, ch, hid), f32), DMA((SLOTS,))],
        compiler_params=params(8),
        name="feedback",
    )(*args)


WSLOTS = 4


def update_kernel(at_ref, w_ref, raw_ref, scale_ref, tok_ref, *rest, other, shares):
    n = shares if other else 1
    if other:
        rest, near_ref, wsem = rest[:-2], rest[-2], rest[-1]
    invs, rights = rest[:n], rest[n : 2 * n]
    out_ref, decs = rest[-6 - shares], rest[-5 - shares : -5]
    inv_ref, right_ref, stage_ref, acc_ref, sem = rest[-5:]
    width = raw_ref.shape[0]
    ch = rows_per_step(width)
    p = at_ref[2] ^ other
    reads = []
    if other:
        for i, r in enumerate(range(0, width, ch)):
            at = pl.ds(r, ch)
            reads.append(pltpu.make_async_copy(w_ref.at[p, at], near_ref.at[at], wsem.at[i]))
            reads[-1].start()
        w_ref = near_ref
    for j in range(n):
        rows = invs[j].shape[0]
        at = pl.ds(pl.multiple_of((at_ref[0] ^ j) * rows, rows), rows) if other else slice(None)
        inv_ref[at, :] = invs[j][...]
        right_ref[at, :] = rights[j][...]
    pending = []
    share = decs[0].shape[0]
    hi, lo = split(inv_ref[...])
    scale = scale_ref[0:1, :]
    right = right_ref[...]
    acc = None
    for r in range(0, width, ch):
        at = pl.ds(r, ch)
        slot = len(pending) % WSLOTS
        if len(pending) >= WSLOTS:
            pending[len(pending) - WSLOTS].wait()
        raw = raw_ref[at, :]
        left = ((dot_t(raw, hi) + dot_t(raw, lo)) * scale).astype(bf16)
        if other:
            reads[r // ch].wait()
        new = w_ref[at, :] - dot(left, right)
        stage_ref[slot] = new
        copy = pltpu.make_async_copy(stage_ref.at[slot], out_ref.at[p, at], sem.at[slot])
        copy.start()
        pending.append(copy)
        part = dot(tok_ref[:, at], new.astype(bf16))
        acc = part if acc is None else acc + part
    acc_ref[...] = acc
    for j, dec in enumerate(decs):
        dec[...] = acc_ref[pl.ds(pl.multiple_of((at_ref[0] ^ j) * share, share), share), :]
    for copy in pending[-WSLOTS:]:
        copy.wait()


def update(place, w, raw, scale, tokens, invs, rights, out, shares):
    width, half = w.shape[-2:]
    rank = raw.shape[1]
    ch = rows_per_step(width)
    other = out is not None
    args = (place, w, raw, scale, tokens, *invs, *rights) + ((out,) if other else ())
    batch = tokens.shape[0]
    new, *decs = pl.pallas_call(
        functools.partial(update_kernel, other=int(other), shares=shares),
        out_shape=(pltpu.HBM((2, width, half), f32),)
        + (pltpu.VMEM((batch // shares, half), f32),) * shares,
        in_specs=[SM, HB if other else VM]
        + [VM] * (3 + len(invs) + len(rights))
        + ([HB] if other else []),
        out_specs=(HB,) + (VM,) * shares,
        input_output_aliases={len(args) - 1: 0} if other else {},
        scratch_shapes=[
            pltpu.VMEM((rank, rank), f32),
            pltpu.VMEM((rank, half), bf16),
            pltpu.VMEM((WSLOTS, ch, half), f32),
            pltpu.VMEM((batch, half), f32),
            DMA((WSLOTS,)),
        ]
        + ([pltpu.VMEM((width, half), f32), DMA((width // ch,))] if other else []),
        compiler_params=params(18 if other else 9),
        name="update_other" if other else "update_own",
    )(*args)
    return new, decs


def finish_kernel(at_ref, *refs):
    n = (len(refs) - 1) // 2
    own, other = refs[0][...], refs[n][...]
    for k in range(1, n):
        own = own + refs[k][...]
        other = other + refs[n + k][...]
    first = at_ref[2] == 0
    gate, up = jnp.where(first, own, other), jnp.where(first, other, own)
    refs[-1][...] = (gate / (1.0 + jnp.exp(-gate)) * up).astype(bf16)


def finish(place, own, other):
    return pl.pallas_call(
        finish_kernel,
        out_shape=jax.ShapeDtypeStruct(own[0].shape, bf16),
        in_specs=[SM] + [VM] * (len(own) + len(other)),
        out_specs=VM,
        compiler_params=params(4),
        name="finish",
    )(place, *own, *other)


def make_local(nrow, ncol, ngrp):
    def local(momentum, gradient, factor_q, weights, tokens):
        return step(momentum, gradient, factor_q, weights, tokens)

    def step(momentum, gradient, factor_q, weights, tokens):
        row = lax.axis_index("row")
        place = jnp.stack([row, lax.axis_index("col"), lax.axis_index("grp")]).astype(jnp.int32)
        width, hid = momentum.shape[1], momentum.shape[2]
        swap = peers(ngrp, 1)
        q_h = gather_blocks(factor_q[0].astype(bf16), "row", nrow, row, 1)
        buffer, parts = load_left(place, momentum[0], gradient[0], q_h, ncol)
        parts = [parts[k] for k in range(ncol)]
        got = send_all(parts, "col", ncol)
        weights = in_hbm(weights)
        w_own = fetch(place, weights, parts[0])
        block = block_sum([parts[0]] + got)
        raw, gram = join_gram(place, [block] + send_all([block] * ncol, "col", ncol))
        raw_other = lax.ppermute(raw, "grp", swap)
        gram = sum_over(gram, "row", nrow)
        rr, rr_h = raw_right(raw, buffer)
        for k in bits_of(nrow)[:-1]:
            rr = rr + lax.ppermute(rr_h, "row", peers(nrow, k)).astype(f32)
            rr_h = rr.astype(bf16)
        rr_other = lax.ppermute(rr_h, "row", peers(nrow, bits_of(nrow)[-1]))
        inv_l, inv_part = chol_inv(place, gram, nrow)
        inv_part = lax.ppermute(inv_part, "grp", swap)
        left_h, right, right_h, right_own, half_part, squares = factors(
            place, raw, inv_l, rr, rr_other, ngrp, nrow
        )
        half_part = lax.ppermute(half_part, "grp", swap)
        rounds = bits_of(ncol)
        cuts = [width * i // 4 for i in range(5)]
        mom_new = None
        for i in range(4):
            mom_new = apply_feedback(buffer, left_h, right_h, mom_new, cuts[i], cuts[i + 1])
        for k in rounds:
            squares = squares + lax.ppermute(squares, "col", peers(ncol, k))
        step_size = 0.4 * math.sqrt(max(width * nrow, hid * ncol))
        inv_norm = 1.0 / jnp.sqrt(squares + epsilon)
        inv_norm_other = lax.ppermute(inv_norm, "grp", swap)
        q_share = factor_share(place, right, inv_norm, factor_q.shape[2])
        scale, mom_new = lax.optimization_barrier((step_size * inv_norm, mom_new))
        new_weights, dec = update(
            place, w_own, raw, scale, tokens, [inv_l], [right_own], None, nrow
        )
        inv_part, half_part, mom_new = lax.optimization_barrier(
            (inv_part, half_part, mom_new)
        )
        invs = [inv_part] + send_all([inv_part] * nrow, "row", nrow)
        halves = [half_part] + send_all([half_part] * nrow, "row", nrow)
        new_weights, dec_other = update(
            place, weights, raw_other, step_size * inv_norm_other, tokens, invs, halves,
            new_weights, nrow,
        )
        dec[1:] = send_all(dec, "row", nrow)
        dec_other[1:] = send_all(dec_other, "row", nrow)
        hidden = finish(place, dec, dec_other)
        return (mom_new[None], q_share[None], new_weights, hidden)

    return local


def solution(mesh):
    in_specs = (
        P("grp", "row", "col"),
        P("grp", "row", "col"),
        P("grp", "col", "row"),
        P(None, "row", ("col", "grp")),
        P(None, "row"),
    )
    out_specs = (
        P("grp", "row", "col"),
        P("grp", "col", "row"),
        P(None, "row", ("col", "grp")),
        P("row", ("col", "grp")),
    )
    local = make_local(mesh.shape["row"], mesh.shape["col"], mesh.shape["grp"])
    return jax.shard_map(local, mesh=mesh, in_specs=in_specs, out_specs=out_specs, check_vma=False)
```

```python
import functools
import math

import jax
import jax.numpy as jnp
from jax import lax
from jax.experimental import pallas as pl
from jax.experimental.pallas import tpu as pltpu
from jax.sharding import PartitionSpec as P


feedback = 0.05
epsilon = 1e-06

f32 = jnp.float32
bf16 = jnp.bfloat16


def peers(n, k):
    return [(i, i ^ k) for i in range(n)]


def bits_of(n):
    assert n & (n - 1) == 0
    return [1 << b for b in range(n.bit_length() - 1)]


def gather_blocks(x, axis, n, at, dim):
    for k in bits_of(n):
        other = lax.ppermute(x, axis, peers(n, k))
        upper = (at & k) != 0
        x = jnp.concatenate([jnp.where(upper, other, x), jnp.where(upper, x, other)], axis=dim)
    return x


def sum_over(x, axis, n, wire=f32):
    for k in bits_of(n):
        x = x + lax.ppermute(x.astype(wire), axis, peers(n, k)).astype(f32)
    return x


def send_all(blocks, axis, n):
    return [lax.ppermute(blocks[k], axis, peers(n, k)) for k in range(1, n)]


class Grid:
    def __init__(self, n, size):
        self.n, self.size = n, size
        self.nx = max(x for x in bits_of(n) + [n] if x * x <= n)
        self.nz = n // self.nx
        self.head = size if size < 48 else (size * 2 // 3 + 15) // 16 * 16
        self.tail = size - self.head

    def send_x(self, blocks):
        return [lax.ppermute(b, "col", peers(self.n, k)) for k, b in enumerate(blocks, 1)]

    def send_z(self, blocks):
        return [lax.ppermute(b, "col", peers(self.n, k * self.nx)) for k, b in enumerate(blocks, 1)]


def ds(i, n):
    return slice(i * n, (i + 1) * n)


def stacked(x, order):
    one = x.astype(bf16)
    rest = x - one.astype(f32)
    two = rest.astype(bf16)
    pieces = (one, two, (rest - two.astype(f32)).astype(bf16))
    return jnp.concatenate([pieces[i] for i in order], axis=0)


def chol_inv_kernel(at_ref, g_ref, out_ref, part_ref, s_ref):
    n = g_ref.shape[0]
    b = 16
    s_ref[:, :n] = g_ref[...]
    s_ref[:, n:] = (
        lax.broadcasted_iota(jnp.int32, (n, n), 0) == lax.broadcasted_iota(jnp.int32, (n, n), 1)
    ).astype(f32)
    rows = lax.broadcasted_iota(jnp.int32, (b, 128), 0)
    for r0 in range(0, n, b):
        lo = r0 // 128 * 128
        hi = n + (r0 + b + 127) // 128 * 128
        tiles = [s_ref[r0 : r0 + b, t : t + 128] for t in range(lo, hi, 128)]
        cols = [
            jnp.broadcast_to(tiles[0][:, r0 - lo + j : r0 - lo + j + 1], (b, 128)) for j in range(b)
        ]
        scale = None
        for i in range(b):
            piv = jnp.broadcast_to(cols[i][i : i + 1, :], (b, 128))
            scale = piv if scale is None else jnp.where(rows == i, piv, scale)
            if i + 1 < b:
                ratio = jnp.where(rows > i, cols[i], 0.0) * (1.0 / piv)
                for j in range(i + 1, b):
                    cols[j] = cols[j] - ratio * cols[j][i : i + 1, :]
                tiles = [t - ratio * t[i : i + 1, :] for t in tiles]
        scale = lax.rsqrt(scale)
        tiles = [t * scale for t in tiles]
        if r0 + b < n:
            upper = jnp.concatenate(tiles, axis=1)
            upd = dot(
                stacked(upper[:, : n - lo], (0, 0, 1, 0, 1, 2)).T,
                stacked(upper, (0, 1, 0, 2, 1, 0)),
            )
            s_ref[r0 + b :, lo:hi] = s_ref[r0 + b :, lo:hi] - upd[r0 + b - lo :, :]
        for k, t in enumerate(range(lo, hi, 128)):
            if t >= n:
                out_ref[r0 : r0 + b, t - n : t - n + 128] = tiles[k]
        for t in range(hi, 2 * n, 128):
            out_ref[r0 : r0 + b, t - n : t - n + 128] = jnp.zeros((b, 128), f32)
    rows = part_ref.shape[0]
    part_ref[...] = out_ref[pl.ds(pl.multiple_of(at_ref[0] * rows, rows), rows), :]


def chol_inv(place, gram, shares):
    n = gram.shape[0]
    return pl.pallas_call(
        chol_inv_kernel,
        out_shape=(pltpu.VMEM((n, n), f32), pltpu.VMEM((n // shares, n), f32)),
        in_specs=[SM, VM],
        out_specs=(VM, VM),
        scratch_shapes=[pltpu.VMEM((n, 2 * n), f32)],
        compiler_params=params(6),
        name="chol_inv",
    )(place, gram)


def split(x):
    hi = x.astype(bf16)
    return hi, (x - hi.astype(f32)).astype(bf16)


def dot_t(a, b):
    return lax.dot_general(a, b, (((1,), (1,)), ((), ())), preferred_element_type=f32)


def dot(a, b):
    return jnp.dot(a, b, preferred_element_type=f32)


VM = pl.BlockSpec(memory_space=pltpu.VMEM)
SM = pl.BlockSpec(memory_space=pltpu.SMEM)
HB = pl.BlockSpec(memory_space=pltpu.HBM)
DMA = pltpu.SemaphoreType.DMA


def params(mib):
    return pltpu.CompilerParams(vmem_limit_bytes=mib << 20)


def rows_per_step(width):
    return min(256, width)


def load_kernel(at_ref, m_ref, g_ref, q_ref, buf_ref, *rest, grid):
    outs = rest[:-4]
    left_ref, grad_ref, sem_m, sem_g = rest[-4:]
    width = buf_ref.shape[0]
    _, size, _ = left_ref.shape
    ch = rows_per_step(width)
    copies = []
    for i in range(width // ch):
        at = pl.ds(i * ch, ch)
        pair = (
            pltpu.make_async_copy(m_ref.at[at], buf_ref.at[at], sem_m.at[i]),
            pltpu.make_async_copy(g_ref.at[at], grad_ref.at[at], sem_g.at[i]),
        )
        for c in pair:
            c.start()
        copies.append(pair)
    for i, pair in enumerate(copies):
        at = pl.ds(i * ch, ch)
        for c in pair:
            c.wait()
        buf = buf_ref[at, :] + grad_ref[at, :].astype(f32)
        buf_ref[at, :] = buf
        part = dot(buf.astype(bf16), q_ref[...]).astype(bf16)
        for r in range(0, ch, size):
            left_ref[at_ref[1] ^ ((i * ch + r) // size)] = part[r : r + size, :]
    for x in range(grid.nx):
        for z in range(grid.nz):
            outs[x][ds(z, grid.head), :] = left_ref[x + grid.nx * z, : grid.head, :]
    if grid.tail:
        for z in range(grid.nz):
            for x in range(grid.nx):
                outs[grid.nx + z][ds(x, grid.tail), :] = left_ref[x + grid.nx * z, grid.head :, :]


def load_left(place, m, g, q, grid):
    width, hid = m.shape
    rank = q.shape[1]
    blocks = grid.n
    n = width // rows_per_step(width)
    assert rows_per_step(width) % (width // blocks) == 0
    outs = [pltpu.VMEM((grid.nz * grid.head, rank), bf16)] * grid.nx
    if grid.tail:
        outs += [pltpu.VMEM((grid.nx * grid.tail, rank), bf16)] * grid.nz
    buf, *outs = pl.pallas_call(
        functools.partial(load_kernel, grid=grid),
        out_shape=(pltpu.VMEM((width, hid), f32), *outs),
        in_specs=[SM, HB, HB, VM],
        out_specs=(VM,) * (1 + len(outs)),
        scratch_shapes=[
            pltpu.VMEM((blocks, width // blocks, rank), bf16),
            pltpu.VMEM((width, hid), bf16),
            DMA((n,)),
            DMA((n,)),
        ],
        compiler_params=params(16),
        name="load_left",
    )(place, in_hbm(m), in_hbm(g), q)
    return buf, outs[: grid.nx], outs[grid.nx :]


def in_hbm(x):
    return pltpu.with_memory_space_constraint(x, pltpu.HBM)


def fetch_kernel(at_ref, w_ref, after_ref, out_ref, sem, *, other):
    copies = []
    ch = rows_per_step(w_ref.shape[1])
    for i in range(w_ref.shape[1] // ch):
        at = pl.ds(i * ch, ch)
        copies.append(
            pltpu.make_async_copy(w_ref.at[at_ref[2] ^ other, at], out_ref.at[at], sem.at[i])
        )
    for c in copies:
        c.start()
    for c in copies:
        c.wait()


def fetch(place, w, after, other):
    n = w.shape[1] // rows_per_step(w.shape[1])
    return pl.pallas_call(
        functools.partial(fetch_kernel, other=other),
        out_shape=pltpu.VMEM(w.shape[1:], w.dtype),
        in_specs=[SM, HB, VM],
        out_specs=VM,
        scratch_shapes=[DMA((n,))],
        compiler_params=params(1),
        name="fetch_weights",
    )(place, w, after)


def add_up(refs, rows):
    total = refs[0][rows, :].astype(f32)
    for r in refs[1:]:
        total = total + r[rows, :].astype(f32)
    return total.astype(bf16)


def halfway_kernel(*refs, grid):
    heads, tails = refs[: grid.nx], refs[grid.nx : grid.nx + (grid.nz if grid.tail else 0)]
    outs = refs[len(heads) + len(tails) :]
    for z in range(grid.nz):
        outs[z][...] = add_up(heads, ds(z, grid.head))
    if grid.tail:
        for x in range(grid.nx):
            outs[grid.nz + x][...] = add_up(tails, ds(x, grid.tail))


def halfway(grid, heads, tails):
    rank = heads[0].shape[1]
    outs = [pltpu.VMEM((grid.head, rank), bf16)] * grid.nz
    if grid.tail:
        outs += [pltpu.VMEM((grid.tail, rank), bf16)] * grid.nx
    outs = pl.pallas_call(
        functools.partial(halfway_kernel, grid=grid),
        out_shape=tuple(outs),
        in_specs=[VM] * (len(heads) + len(tails)),
        out_specs=(VM,) * len(outs),
        compiler_params=params(4),
        name="halfway",
    )(*heads, *tails)
    return list(outs[: grid.nz]), list(outs[grid.nz :])


def block_kernel(*refs, grid):
    n = grid.nz
    refs[-2 if grid.tail else -1][...] = add_up(refs[:n], slice(None))
    if grid.tail:
        refs[-1][...] = add_up(refs[n : n + grid.nx], slice(None))


def block_sum(grid, heads, tails):
    rank = heads[0].shape[1]
    outs = [pltpu.VMEM((grid.head, rank), bf16)]
    if grid.tail:
        outs += [pltpu.VMEM((grid.tail, rank), bf16)]
    outs = pl.pallas_call(
        functools.partial(block_kernel, grid=grid),
        out_shape=tuple(outs),
        in_specs=[VM] * (len(heads) + len(tails)),
        out_specs=(VM,) * len(outs),
        compiler_params=params(4),
        name="block_sum",
    )(*heads, *tails)
    return outs[0], (outs[1] if grid.tail else None)


def stack_kernel(*refs, sizes):
    outs = refs[-len(sizes) :]
    at = 0
    for out, n in zip(outs, sizes):
        for k in range(n):
            out[ds(k, refs[at].shape[0]), :] = refs[at][...]
            at += 1


def stack_rows(*groups):
    groups = [g for g in groups if g]
    flat = [b for g in groups for b in g]
    outs = tuple(
        pltpu.VMEM((len(g) * g[0].shape[0], g[0].shape[1]), g[0].dtype) for g in groups
    )
    return pl.pallas_call(
        functools.partial(stack_kernel, sizes=tuple(len(g) for g in groups)),
        out_shape=outs,
        in_specs=[VM] * len(flat),
        out_specs=(VM,) * len(outs),
        compiler_params=params(4),
        name="stack_rows",
    )(*flat)


def gram_kernel(at_ref, *refs, grid):
    heads, tails, (raw_ref, rest_ref, gram_ref) = refs[: grid.nx], refs[grid.nx : -3], refs[-3:]
    spread_rows(at_ref, grid, heads, tails, raw_ref)
    at = 0
    for r in heads[1:] + tails[1:]:
        rest_ref[at : at + r.shape[0], :] = r[...]
        at += r.shape[0]
    raw = raw_ref[...]
    gram_ref[...] = lax.dot_general(
        raw, raw, (((0,), (0,)), ((), ())), preferred_element_type=f32
    )


def join_gram(place, grid, heads, tails):
    rank = heads[0].shape[1]
    rest = sum(r.shape[0] for r in heads[1:] + tails[1:])
    return pl.pallas_call(
        functools.partial(gram_kernel, grid=grid),
        out_shape=(
            pltpu.VMEM((grid.size * grid.n, rank), bf16),
            pltpu.VMEM((rest, rank), bf16),
            pltpu.VMEM((rank, rank), f32),
        ),
        in_specs=[SM] + [VM] * (len(heads) + len(tails)),
        out_specs=(VM, VM, VM),
        compiler_params=params(6),
        name="join_gram",
    )(place, *heads, *tails)


def sum_scatter_gather(place, grid, heads, tails, swap, cover):
    got_z = grid.send_z(tails[1:])
    got_x = grid.send_x(heads[1:])
    own = cover(heads[0], 0)
    heads, tails = halfway(grid, heads[:1] + got_x, tails[:1] + got_z)
    got_z = grid.send_z(heads[1:])
    got_x = grid.send_x(tails[1:])
    head, tail = block_sum(grid, heads[:1] + got_z, tails[:1] + got_x)
    heads = [head] + grid.send_z([head] * (grid.nz - 1))
    tails = [tail] + grid.send_x([tail] * (grid.nx - 1)) if grid.tail else []
    other = cover(head, 1)
    stacks = stack_rows(heads, tails)
    raws = [lax.ppermute(x, "grp", swap) for x in stacks]
    tails = grid.send_z([stacks[1]] * (grid.nz - 1)) if grid.tail else []
    heads = [stacks[0]] + grid.send_x([stacks[0]] * (grid.nx - 1))
    if grid.tail:
        tails = [stacks[1]] + tails
    raw, rest, gram = join_gram(place, grid, heads, tails)
    raws.append(lax.ppermute(rest, "grp", swap))
    return raw, gram, raws, own, other


def right_kernel(raw_ref, buf_ref, out_ref, outh_ref):
    raw_t = raw_ref[...].T
    hid = buf_ref.shape[1]
    ch = min(256, hid)
    for i in range(hid // ch):
        at = pl.ds(i * ch, ch)
        part = dot(raw_t, buf_ref[:, at].astype(bf16))
        out_ref[:, at] = part
        outh_ref[:, at] = part.astype(bf16)


def raw_right(raw, buf):
    shape = (raw.shape[1], buf.shape[1])
    return pl.pallas_call(
        right_kernel,
        out_shape=(pltpu.VMEM(shape, f32), pltpu.VMEM(shape, bf16)),
        in_specs=[VM, VM],
        out_specs=(VM, VM),
        compiler_params=params(6),
        name="raw_right",
    )(raw, buf)


def factors_kernel(
    at_ref, raw_ref, inv_ref, rr_ref, rro_ref, leftf_ref, left_ref, right_ref, righth_ref, own_ref, part_ref, sq_ref,
    split_ref,
):
    inv_hi, inv_lo = split(inv_ref[...])
    left = dot_t(raw_ref[...], inv_hi) + dot_t(raw_ref[...], inv_lo)
    leftf_ref[...] = left
    left_ref[...] = left.astype(bf16)
    hid = rr_ref.shape[1]
    half = split_ref.shape[2]
    ch = min(512, half)
    total = jnp.zeros((rr_ref.shape[0], 1), f32)
    for i in range(hid // ch):
        at = pl.ds(i * ch, ch)
        hi, lo = split(rr_ref[:, at] + rro_ref[:, at].astype(f32))
        right = dot(inv_hi, hi) + dot(inv_lo, hi) + dot(inv_hi, lo)
        right_ref[:, at] = right
        right_h = right.astype(bf16)
        righth_ref[:, at] = right_h
        split_ref[at_ref[2] ^ (i * ch // half), :, pl.ds(i * ch % half, ch)] = right_h
        total = total + jnp.sum(right * right, axis=1, keepdims=True)
    own_ref[...] = split_ref[0]
    rows = part_ref.shape[0]
    part_ref[...] = split_ref[1, pl.ds(pl.multiple_of(at_ref[0] * rows, rows), rows), :]
    sq_ref[...] = jnp.broadcast_to(total, (total.shape[0], 128)).T[: sq_ref.shape[0], :]


def factors(place, raw, inv_l, rr, rro, groups, shares):
    rank, hid = rr.shape
    return pl.pallas_call(
        factors_kernel,
        out_shape=(
            pltpu.VMEM(raw.shape, f32),
            pltpu.VMEM(raw.shape, bf16),
            pltpu.VMEM((rank, hid), f32),
            pltpu.VMEM((rank, hid), bf16),
            pltpu.VMEM((rank, hid // groups), bf16),
            pltpu.VMEM((rank // shares, hid // groups), bf16),
            pltpu.VMEM((8, rank), f32),
        ),
        in_specs=[SM, VM, VM, VM, VM],
        out_specs=(VM,) * 7,
        scratch_shapes=[pltpu.VMEM((groups, rank, hid // groups), bf16)],
        compiler_params=params(6),
        name="factors",
    )(place, raw, inv_l, rr, rro)


def share_kernel(at_ref, right_ref, norm_ref, out_ref, col_ref):
    n = out_ref.shape[1]
    col_ref[...] = norm_ref[...].T
    at = pl.ds(pl.multiple_of(at_ref[0] * n, n), n)
    out_ref[...] = (right_ref[at, :] * col_ref[at, 0:1]).T


def factor_share(place, right, inv_norm, share):
    rank, hid = right.shape
    return pl.pallas_call(
        share_kernel,
        out_shape=jax.ShapeDtypeStruct((hid, share), f32),
        in_specs=[SM, VM, VM],
        out_specs=VM,
        scratch_shapes=[pltpu.VMEM((rank, 8), f32)],
        compiler_params=params(6),
        name="factor_share",
    )(place, right, inv_norm)


SLOTS = 4


def feedback_kernel(buf_ref, left_ref, right_ref, *rest, lo, hi, ch):
    out_ref, stage_ref, sem = rest[-3:]
    pending = []
    for i, r in enumerate(range(lo, hi, ch)):
        slot = i % SLOTS
        if i >= SLOTS:
            pending[i - SLOTS].wait()
        at = pl.ds(r, ch)
        stage_ref[slot] = buf_ref[at, :] - feedback * dot(left_ref[at, :], right_ref[...])
        copy = pltpu.make_async_copy(stage_ref.at[slot], out_ref.at[at], sem.at[slot])
        copy.start()
        pending.append(copy)
    for copy in pending[-SLOTS:]:
        copy.wait()


def apply_feedback(buf, left, right, out, lo, hi):
    width, hid = buf.shape
    ch = min(128, hi - lo)
    args = (buf, left, right) + (() if out is None else (out,))
    return pl.pallas_call(
        functools.partial(feedback_kernel, lo=lo, hi=hi, ch=ch),
        out_shape=pltpu.HBM((width, hid), f32),
        in_specs=[VM, VM, VM] + ([] if out is None else [HB]),
        out_specs=HB,
        input_output_aliases={} if out is None else {3: 0},
        scratch_shapes=[pltpu.VMEM((SLOTS, ch, hid), f32), DMA((SLOTS,))],
        compiler_params=params(8),
        name="feedback",
    )(*args)


WSLOTS = 3


def spread_rows(at_ref, grid, heads, tails, out_ref):
    for x in range(grid.nx):
        for z in range(grid.nz):
            start = (at_ref[1] ^ (x + grid.nx * z)) * grid.size
            at = pl.ds(pl.multiple_of(start, 16), grid.head)
            out_ref[at, :] = heads[x][ds(z, grid.head), :]
            if grid.tail:
                at = pl.ds(pl.multiple_of(start + grid.head, 16), grid.tail)
                out_ref[at, :] = tails[z][ds(x, grid.tail), :]


def update_rows(p, w_ref, left_of, right, tok_ref, out_ref, stage_ref, sem):
    width = w_ref.shape[0]
    ch = stage_ref.shape[1]
    pending = []
    acc = None
    for r in range(0, width, ch):
        at = pl.ds(r, ch)
        slot = len(pending) % WSLOTS
        if len(pending) >= WSLOTS:
            pending[len(pending) - WSLOTS].wait()
        new = w_ref[at, :] - dot(left_of(at), right)
        stage_ref[slot] = new
        copy = pltpu.make_async_copy(stage_ref.at[slot], out_ref.at[p, at], sem.at[slot])
        copy.start()
        pending.append(copy)
        part = dot(tok_ref[:, at], new.astype(bf16))
        acc = part if acc is None else acc + part
    return acc, pending[-WSLOTS:]


def split_decode(at_ref, acc, acc_ref, decs):
    share = decs[0].shape[0]
    acc_ref[...] = acc
    for j, dec in enumerate(decs):
        dec[...] = acc_ref[pl.ds(pl.multiple_of((at_ref[0] ^ j) * share, share), share), :]


def own_kernel(at_ref, w_ref, left_ref, scale_ref, right_ref, tok_ref, out_ref, *rest):
    decs, (stage_ref, acc_ref, sem) = rest[:-3], rest[-3:]
    scale = scale_ref[0:1, :]
    acc, pending = update_rows(
        at_ref[2],
        w_ref,
        lambda at: (left_ref[at, :] * scale).astype(bf16),
        right_ref[...],
        tok_ref,
        out_ref,
        stage_ref,
        sem,
    )
    split_decode(at_ref, acc, acc_ref, decs)
    for copy in pending:
        copy.wait()


def other_kernel(at_ref, w_ref, scale_ref, tok_ref, *rest, grid, shares):
    invs, rest = rest[:shares], rest[shares:]
    rights, rest = rest[:shares], rest[shares:]
    raws, out_ref, decs = rest[: -8 - shares], rest[-7 - shares], rest[-6 - shares : -6]
    inv_ref, right_ref, raw_ref, stage_ref, acc_ref, sem = rest[-6:]
    rows = invs[0].shape[0]
    for j in range(shares):
        at = pl.ds(pl.multiple_of((at_ref[0] ^ j) * rows, rows), rows)
        inv_ref[at, :] = invs[j][...]
        right_ref[at, :] = rights[j][...]
    spread_parts(at_ref, grid, raws, raw_ref)
    hi, lo = split(inv_ref[...])
    scale = scale_ref[0:1, :]

    def left_of(at):
        raw = raw_ref[at, :]
        return ((dot_t(raw, hi) + dot_t(raw, lo)) * scale).astype(bf16)

    acc, pending = update_rows(
        at_ref[2] ^ 1, w_ref, left_of, right_ref[...], tok_ref, out_ref, stage_ref, sem
    )
    split_decode(at_ref, acc, acc_ref, decs)
    for copy in pending:
        copy.wait()


def spread_parts(at_ref, grid, raws, out_ref):
    first, (rest_ref,) = raws[:-1], raws[-1:]
    n, m = grid.nz * grid.head, grid.nx * grid.tail
    heads = [first[0]] + [rest_ref.at[ds(k, n)] for k in range(grid.nx - 1)]
    base = (grid.nx - 1) * n
    tails = []
    if grid.tail:
        tails = [first[1]] + [
            rest_ref.at[slice(base + k * m, base + (k + 1) * m)] for k in range(grid.nz - 1)
        ]
    spread_rows(at_ref, grid, heads, tails, out_ref)


def update_shapes(w, tokens, shares):
    width, half = w.shape
    batch = tokens.shape[0]
    outs = (pltpu.HBM((2, width, half), f32),) + (pltpu.VMEM((batch // shares, half), f32),) * shares
    scratch = [
        pltpu.VMEM((WSLOTS, min(512, width), half), f32),
        pltpu.VMEM((batch, half), f32),
        DMA((WSLOTS,)),
    ]
    return outs, (HB,) + (VM,) * shares, scratch


def update_own(place, w, left, scale, right, tokens, shares):
    outs, specs, scratch = update_shapes(w, tokens, shares)
    new, *decs = pl.pallas_call(
        own_kernel,
        out_shape=outs,
        in_specs=[SM] + [VM] * 5,
        out_specs=specs,
        scratch_shapes=scratch,
        compiler_params=params(12),
        name="update_own",
    )(place, w, left, scale, right, tokens)
    return new, decs


def update_other(place, grid, w, scale, tokens, invs, rights, raws, out, shares):
    outs, specs, scratch = update_shapes(w, tokens, shares)
    args = (place, w, scale, tokens, *invs, *rights, *raws, out)
    rank = scale.shape[1]
    new, *decs = pl.pallas_call(
        functools.partial(other_kernel, grid=grid, shares=shares),
        out_shape=outs,
        in_specs=[SM] + [VM] * (len(args) - 2) + [HB],
        out_specs=specs,
        input_output_aliases={len(args) - 1: 0},
        scratch_shapes=[
            pltpu.VMEM((rank, rank), f32),
            pltpu.VMEM((rank, w.shape[1]), bf16),
            pltpu.VMEM((w.shape[0], rank), bf16),
        ]
        + scratch,
        compiler_params=params(14),
        name="update_other",
    )(*args)
    return new, decs


def finish_kernel(at_ref, *refs):
    n = (len(refs) - 1) // 2
    own, other = refs[0][...], refs[n][...]
    for k in range(1, n):
        own = own + refs[k][...]
        other = other + refs[n + k][...]
    first = at_ref[2] == 0
    gate, up = jnp.where(first, own, other), jnp.where(first, other, own)
    refs[-1][...] = (gate / (1.0 + jnp.exp(-gate)) * up).astype(bf16)


def finish(place, own, other):
    return pl.pallas_call(
        finish_kernel,
        out_shape=jax.ShapeDtypeStruct(own[0].shape, bf16),
        in_specs=[SM] + [VM] * (len(own) + len(other)),
        out_specs=VM,
        compiler_params=params(4),
        name="finish",
    )(place, *own, *other)


def make_local(nrow, ncol, ngrp):
    def local(momentum, gradient, factor_q, weights, tokens):
        return step(momentum, gradient, factor_q, weights, tokens)

    def step(momentum, gradient, factor_q, weights, tokens):
        row = lax.axis_index("row")
        place = jnp.stack([row, lax.axis_index("col"), lax.axis_index("grp")]).astype(jnp.int32)
        width, hid = momentum.shape[1], momentum.shape[2]
        swap = peers(ngrp, 1)
        q_h = gather_blocks(factor_q[0].astype(bf16), "row", nrow, row, 1)
        grid = Grid(ncol, width // ncol)
        weights = in_hbm(weights)
        buffer, heads, tails = load_left(place, momentum[0], gradient[0], q_h, grid)

        raw, gram, raws, w_own, w_other = sum_scatter_gather(
            place, grid, heads, tails, swap, lambda after, s: fetch(place, weights, after, s)
        )
        gram = sum_over(gram, "row", nrow)
        rr, rr_h = raw_right(raw, buffer)
        for k in bits_of(nrow)[:-1]:
            rr = rr + lax.ppermute(rr_h, "row", peers(nrow, k)).astype(f32)
            rr_h = rr.astype(bf16)
        rr_other = lax.ppermute(rr_h, "row", peers(nrow, bits_of(nrow)[-1]))
        inv_l, inv_part = chol_inv(place, gram, nrow)
        inv_part = lax.ppermute(inv_part, "grp", swap)
        left, left_h, right, right_h, right_own, half_part, squares = factors(
            place, raw, inv_l, rr, rr_other, ngrp, nrow
        )
        half_part = lax.ppermute(half_part, "grp", swap)
        rounds = bits_of(ncol)
        cuts = [width * i // 4 for i in range(5)]
        mom_new = None
        for i in range(4):
            mom_new = apply_feedback(buffer, left_h, right_h, mom_new, cuts[i], cuts[i + 1])
        for k in rounds:
            squares = squares + lax.ppermute(squares, "col", peers(ncol, k))
        step_size = 0.4 * math.sqrt(max(width * nrow, hid * ncol))
        inv_norm = 1.0 / jnp.sqrt(squares + epsilon)
        inv_norm_other = lax.ppermute(inv_norm, "grp", swap)
        q_share = factor_share(place, right, inv_norm, factor_q.shape[2])
        scale, mom_new = lax.optimization_barrier((step_size * inv_norm, mom_new))
        new_weights, dec = update_own(place, w_own, left, scale, right_own, tokens, nrow)
        inv_part, half_part, mom_new = lax.optimization_barrier(
            (inv_part, half_part, mom_new)
        )
        invs = [inv_part] + send_all([inv_part] * nrow, "row", nrow)
        halves = [half_part] + send_all([half_part] * nrow, "row", nrow)
        new_weights, dec_other = update_other(
            place, grid, w_other, step_size * inv_norm_other, tokens, invs, halves, raws,
            new_weights, nrow,
        )
        dec[1:] = send_all(dec, "row", nrow)
        dec_other[1:] = send_all(dec_other, "row", nrow)
        hidden = finish(place, dec, dec_other)
        return (mom_new[None], q_share[None], new_weights, hidden)

    return local


def solution(mesh):
    in_specs = (
        P("grp", "row", "col"),
        P("grp", "row", "col"),
        P("grp", "col", "row"),
        P(None, "row", ("col", "grp")),
        P(None, "row"),
    )
    out_specs = (
        P("grp", "row", "col"),
        P("grp", "col", "row"),
        P(None, "row", ("col", "grp")),
        P("row", ("col", "grp")),
    )
    local = make_local(mesh.shape["row"], mesh.shape["col"], mesh.shape["grp"])
    return jax.shard_map(local, mesh=mesh, in_specs=in_specs, out_specs=out_specs, check_vma=False)
```
